32 devices in a mesh: slab: 2 (over core), py: 4 (over z), pz: 4 (over y, x).
Axes of the slice: x: 2, y: 2, z: 4, core: 2. Of those that a mesh axis runs over, the one named last changes fastest.
Arguments:
- start_vector: float32 [32, 128, 256], P('pz', 'py', 'slab'), may hold values from -6 to 6
- potential: float32 [32, 128, 256], P('pz', 'py', 'slab'), may hold values from 0.5 to 4
Outputs:
- krylov_basis: float32 [6, 32, 128, 256], P(None, 'pz', 'py', 'slab')
- tridiagonal: float32 [2, 5], replicated
The draws below stay inside these ranges and needn't reach their ends.
All inputs are finite; a program needn't handle non-finite values.
Results may differ from the reference program's by a relative error of at most 0.00012.
Values sent between devices are 32-bit elements; how exact they have to be, the bound alone decides.
A program may use at most 64 MiB of HBM per device.

```python
import jax
import jax.numpy as jnp
from jax import lax

ITERS = 5
NX = 256
NY = 128
NZ = 32


def level_of(key, dims, shards, smallest, top_value):
    loudness = 1.0
    for position, parts in shards:
        steps = jax.random.uniform(jax.random.fold_in(jax.random.fold_in(key, 6), position), (parts,), jnp.float32, smallest / len(shards), top_value / len(shards))
        loudness = loudness * jnp.repeat(jnp.exp(steps), dims[position] // parts).reshape((-1,) + (1,) * (len(dims) - 1 - position))
    return loudness


def normal_values(key, shape, deviation, limit, split=(), dtype=jnp.bfloat16):
    values = jax.random.normal(key, shape, jnp.float32) * deviation
    if len(split) > 0:
        values = level_of(key, shape, split, -0.22, 0.18) * values
    return jnp.clip(values, min=-limit, max=limit).astype(dtype)


def setup_inputs(seed: int = 0) -> dict:
    key_of = jax.random.split(jax.random.key(seed), 3)
    return {
        "start_vector": normal_values(key_of[0], (NZ, NY, NX), 1.0, 6.0, ((0, 4), (1, 4), (2, 2)), jnp.float32),
        "potential": jnp.clip(0.5 + 3.5 * jax.random.uniform(key_of[1], (NZ, NY, NX), jnp.float32) ** level_of(key_of[1], (NZ, NY, NX), ((0, 4), (1, 4), (2, 2)), -0.2, 0.2), 0.5, 4.0),
    }


EPSILON = 1e-06

def apply_hamiltonian(field, potential):
    padded = jnp.pad(field, 1)
    beside = padded[2:, 1:-1, 1:-1] + padded[:-2, 1:-1, 1:-1]
    beside = beside + padded[1:-1, 2:, 1:-1] + padded[1:-1, :-2, 1:-1]
    beside = beside + padded[1:-1, 1:-1, 2:] + padded[1:-1, 1:-1, :-2]
    return (6.0 + potential) * field - beside

def reference(start_vector, potential):
    per_cell = jnp.float32(1.0 / (NX * NY * NZ))
    start_norm = jnp.sum(start_vector * start_vector) * per_cell
    vectors = [start_vector / jnp.sqrt(start_norm + EPSILON)]
    alphas = []
    beta_list = []
    for iteration in range(ITERS):
        image = apply_hamiltonian(vectors[-1], potential)
        active = jnp.stack(vectors)
        first_coeff = jnp.einsum('kzyx,zyx->k', active, image, precision=lax.Precision.HIGHEST) * per_cell
        image = image - jnp.einsum('k,kzyx->zyx', first_coeff, active, precision=lax.Precision.HIGHEST)
        second_coeff = jnp.einsum('kzyx,zyx->k', active, image, precision=lax.Precision.HIGHEST) * per_cell
        image = image - jnp.einsum('k,kzyx->zyx', second_coeff, active, precision=lax.Precision.HIGHEST)
        square_mean = jnp.sum(image * image) * per_cell
        beta_value = jnp.sqrt(square_mean + EPSILON)
        alphas.append(first_coeff[iteration] + second_coeff[iteration])
        beta_list.append(beta_value)
        vectors.append(image / beta_value)
    return (jnp.stack(vectors), jnp.stack([jnp.stack(alphas), jnp.stack(beta_list)]))
```

```python
import functools

import jax
import jax.numpy as jnp
from jax import lax
from jax.experimental import pallas as pl
from jax.experimental.pallas import tpu as pltpu
from jax.sharding import PartitionSpec as P

ITERS = 5
EPSILON = 1e-06
DIAGONAL = 6.0
FIRST_SHIFT = 8.25
MESH = pl.DeviceIdType.MESH
AXES = ("slab", "py", "pz")
UNROLLED = 64


def kernel(sizes, per_cell, x_ref, pot_ref, out_ref, tri_ref, work, ysend, zface, yface, xface,
           rz, ry, rx, slots, send_sem, recv_sem, stat_send, stat_recv):
    Z, Y, X = x_ref.shape
    S, A, B = sizes
    n = S * A * B
    slab, py, pz = (lax.axis_index(name) for name in AXES)
    me = (slab * A + py) * B + pz
    partner = lax.rem(slab + 1, S)

    def to_others(act):
        if n <= UNROLLED:
            slabs = [lax.rem(slab + i, S) for i in range(S)]
            pys = [lax.rem(py + i, A) for i in range(A)]
            pzs = [lax.rem(pz + i, B) for i in range(B)]
            far = sorted(
                ((i, j, k) for i in range(S) for j in range(A) for k in range(B)),
                key=lambda t: -(min(t[1], A - t[1]) + min(t[2], B - t[2])),
            )
            for i, j, k in far:
                if i or j or k:
                    act((slabs[i], pys[j], pzs[k]))
        else:
            def step(d, carry):
                t = lax.rem(me + d, n)
                act((t // (A * B), lax.rem(t // B, A), lax.rem(t, B)))
                return carry
            lax.fori_loop(1, n, step, 0)

    def halo_copies(p, zlo, zhi, block):
        def copy(src, dst, side, target):
            return pltpu.make_async_remote_copy(
                src_ref=src, dst_ref=dst, send_sem=send_sem.at[p, side],
                recv_sem=recv_sem.at[p, side], device_id=target, device_id_type=MESH)
        return (
            (pz < B - 1, pz > 0, copy(zhi, rz.at[p, 0], 0, (slab, py, pz + 1))),
            (pz > 0, pz < B - 1, copy(zlo, rz.at[p, 1], 1, (slab, py, pz - 1))),
            (py < A - 1, py > 0, copy(ysend.at[p, 1], ry.at[p, 0], 2, (slab, py + 1, pz))),
            (py > 0, py < A - 1, copy(ysend.at[p, 0], ry.at[p, 1], 3, (slab, py - 1, pz))),
            (None, None, copy(block, rx.at[p], 4, (partner, py, pz))),
        )

    def when(cond, act):
        if cond is None:
            act()
        else:
            pl.when(cond)(act)

    def exchange(p, zlo, zhi, block):
        copies = halo_copies(p, zlo, zhi, block)
        for sends, _, copy in copies:
            when(sends, copy.start)
        return copies

    def arrived(copies):
        for _, receives, copy in copies:
            when(receives, copy.wait_recv)

    def sent(copies):
        for sends, _, copy in copies:
            when(sends, copy.wait_send)

    def stat_copy(p, target):
        return pltpu.make_async_remote_copy(
            src_ref=slots.at[p, me], dst_ref=slots.at[p, me], send_sem=stat_send.at[p],
            recv_sem=stat_recv.at[p], device_id=target, device_id_type=MESH)

    def wait_all(p, sem):
        span = slots.at[p, pl.ds(0, n - 1)]
        pltpu.make_async_copy(span, span, sem).wait()

    lane = lax.broadcasted_iota(jnp.int32, (Y, X), 1)
    row = lax.broadcasted_iota(jnp.int32, (Y, X), 0)
    has_low = (slab > 0).astype(jnp.float32)
    has_high = (slab < S - 1).astype(jnp.float32)

    def stencil(z, own, zf, yf, xf):
        here = own(z)
        below = own(z - 1) if z > 0 else zf(0)
        above = own(z + 1) if z < Z - 1 else zf(1)
        ylow = jnp.where(row == 0, yf(0, z), pltpu.roll(here, 1, 0))
        yhigh = jnp.where(row == Y - 1, yf(1, z), pltpu.roll(here, Y - 1, 0))
        side = xf(z)
        xlow = pltpu.roll(jnp.where(lane == X - 1, side * has_low, here), 1, 1)
        xhigh = pltpu.roll(jnp.where(lane == 0, side * has_high, here), X - 1, 1)
        return (above + below) + (yhigh + ylow) + (xhigh + xlow)

    def fold(value):
        return jnp.sum(value.reshape(Y // 8, 8, X), axis=0)

    def share(p, sums):
        rows = [jnp.sum(v, axis=0, keepdims=True) for v in sums]
        height = -(-len(rows) // 8) * 8
        rows = rows + [jnp.zeros((1, X), jnp.float32)] * (height - len(rows))
        totals = jnp.sum(jnp.concatenate(rows, axis=0), axis=1, keepdims=True)
        at = lax.broadcasted_iota(jnp.int32, (height, X), 0)
        lanes = lax.broadcasted_iota(jnp.int32, (height, X), 1)
        slots[p, me] = jnp.sum(jnp.where(at == lanes, totals, 0.0), axis=0, keepdims=True)
        to_others(lambda target: stat_copy(p, target).start())

    def gathered(p, count):
        wait_all(p, stat_recv.at[p])
        total = jnp.sum(slots[p], axis=0) * per_cell
        return [jnp.broadcast_to(total[:, s:s + 1], (1, X)) for s in range(count)]

    for p in range(ITERS):
        for side, missing in ((0, pz == 0), (1, pz == B - 1)):
            @pl.when(missing)
            def _(p=p, side=side):
                rz[p, side] = jnp.zeros((Y, X), jnp.float32)
        for side, missing in ((0, py == 0), (1, py == A - 1)):
            @pl.when(missing)
            def _(p=p, side=side):
                ry[p, side] = jnp.zeros((Z, X), jnp.float32)
    for z in range(Z):
        ysend[0, 0, z:z + 1] = x_ref[z, 0:1, :]
        ysend[0, 1, z:z + 1] = x_ref[z, Y - 1:Y, :]

    barrier = pltpu.get_barrier_semaphore()
    to_others(lambda t: pl.semaphore_signal(barrier, inc=1, device_id=t, device_id_type=MESH))
    pl.semaphore_wait(barrier, n - 1)

    pending = [exchange(0, x_ref.at[0], x_ref.at[Z - 1], x_ref)]
    arrived(pending[0])

    gram = {}
    shift, lower = jnp.full((1, X), FIRST_SHIFT, jnp.float32), None
    for j in range(ITERS):
        if j == 0:
            own, zf = (lambda z: x_ref[z]), (lambda s: rz[0, s])
            yf, xf = (lambda s, z: ry[0, s, z:z + 1, :]), (lambda z: rx[0, z])
        else:
            own, zf = (lambda z: out_ref[j, z]), (lambda s: zface[j, s])
            yf, xf = (lambda s, z: yface[j, s, z:z + 1, :]), (lambda z: xface[j, z])
        for z in range(Z):
            image = ((DIAGONAL - shift) + pot_ref[z]) * own(z) - stencil(z, own, zf, yf, xf)
            if j > 0:
                image = image - lower * out_ref[j - 1, z]
            work[j, z] = image
            if j < ITERS - 1:
                ysend[j + 1, 0, z:z + 1] = image[0:1]
                ysend[j + 1, 1, z:z + 1] = image[Y - 1:Y]
        if j < ITERS - 1:
            pending.append(exchange(j + 1, work.at[j, 0], work.at[j, Z - 1], work.at[j]))
        older = [lambda z, k=k: out_ref[k, z] for k in range(j)] + [own]
        sums = [jnp.zeros((8, X), jnp.float32)] * (2 * j + 3)
        for z in range(Z):
            image, newest = work[j, z], own(z)
            for k in range(j + 1):
                v = older[k](z)
                sums[k] = sums[k] + fold(v * image)
                sums[j + 1 + k] = sums[j + 1 + k] + fold(v * newest)
            sums[2 * j + 2] = sums[2 * j + 2] + fold(image * image)
        share(j, sums)
        stats = gathered(j, 2 * j + 3)
        if j == 0:
            scale = 1.0 / jnp.sqrt(stats[1] + EPSILON)
            stats = [s * scale * scale for s in stats]
        a, square = stats[:j + 1], stats[2 * j + 2]
        for k in range(j + 1):
            gram[j, k] = gram[k, j] = stats[j + 1 + k]
        first = [a[k] + shift * gram[k, j] for k in range(j + 1)]
        if j > 0:
            first = [first[k] + lower * gram[k, j - 1] for k in range(j + 1)]
        rest = list(first)
        rest[j] = rest[j] - shift
        if j > 0:
            rest[j - 1] = rest[j - 1] - lower
        coeffs = []
        for k in range(j + 1):
            c = a[k]
            for l in range(j + 1):
                c = c - (gram[k, l] - 1.0 if k == l else gram[k, l]) * rest[l]
            coeffs.append(c)
        for k in range(j + 1):
            along = gram[k, 0] * coeffs[0]
            for l in range(1, j + 1):
                along = along + gram[k, l] * coeffs[l]
            square = square + coeffs[k] * (along - 2.0 * a[k])
        beta = jnp.sqrt(jnp.maximum(square, 0.0) + EPSILON)
        alpha = coeffs[j] + shift
        tri_ref[0:1, j:j + 1] = alpha[:, 0:1]
        tri_ref[1:2, j:j + 1] = beta[:, 0:1]
        inverse = 1.0 / beta

        if j < ITERS - 1:
            arrived(pending[j + 1])

        def follow(vectors, image):
            if j == 0:
                return (image - coeffs[0] * vectors[0]) * (inverse * scale)
            for k in range(j + 1):
                image = image - coeffs[k] * vectors[k]
            return image * inverse

        def step(get, image, put):
            vectors = [get(k) for k in range(j + 1)]
            if j == 0:
                put(0, vectors[0] * scale)
            put(j + 1, follow(vectors, image))

        def putter(ref, *index):
            def put(k, value):
                ref[(k,) + index] = value
            return put

        for z in range(Z):
            step(lambda k: x_ref[z] if j == 0 else out_ref[k, z], work[j, z], putter(out_ref, z))
            if j < ITERS - 1:
                step(lambda k: rx[0, z] if j == 0 else xface[k, z], rx[j + 1, z],
                     putter(xface, z))
        if j < ITERS - 1:
            for s in range(2):
                step(lambda k: rz[0, s] if j == 0 else zface[k, s], rz[j + 1, s],
                     putter(zface, s))
                step(lambda k: ry[0, s] if j == 0 else yface[k, s], ry[j + 1, s],
                     putter(yface, s))
        shift, lower = alpha, beta

    for copies in pending:
        sent(copies)
    for p in range(ITERS):
        wait_all(p, stat_send.at[p])


def shards(sizes, start_vector, potential):
    Z, Y, X = start_vector.shape
    n = sizes[0] * sizes[1] * sizes[2]
    f32 = jnp.float32
    vmem = pl.BlockSpec(memory_space=pltpu.VMEM)
    return tuple(pl.pallas_call(
        functools.partial(kernel, sizes, 1.0 / (start_vector.size * n)),
        out_shape=(jax.ShapeDtypeStruct((ITERS + 1, Z, Y, X), f32),
                   jax.ShapeDtypeStruct((2, ITERS), f32)),
        in_specs=[vmem, vmem],
        out_specs=(vmem, vmem),
        scratch_shapes=[
            pltpu.VMEM((ITERS, Z, Y, X), f32),
            pltpu.VMEM((ITERS, 2, Z, X), f32),
            pltpu.VMEM((ITERS, 2, Y, X), f32),
            pltpu.VMEM((ITERS, 2, Z, X), f32),
            pltpu.VMEM((ITERS, Z, Y, X), f32),
            pltpu.VMEM((ITERS, 2, Y, X), f32),
            pltpu.VMEM((ITERS, 2, Z, X), f32),
            pltpu.VMEM((ITERS, Z, Y, X), f32),
            pltpu.VMEM((ITERS, n, 1, X), f32),
            pltpu.SemaphoreType.DMA((ITERS, 5)),
            pltpu.SemaphoreType.DMA((ITERS, 5)),
            pltpu.SemaphoreType.DMA((ITERS,)),
            pltpu.SemaphoreType.DMA((ITERS,)),
        ],
        compiler_params=pltpu.CompilerParams(collective_id=0, has_side_effects=True),
    )(start_vector, potential))


def solution(mesh):
    sizes = tuple(mesh.shape[name] for name in AXES)
    in_specs = (P("pz", "py", "slab"), P("pz", "py", "slab"))
    out_specs = (P(None, "pz", "py", "slab"), P())
    return jax.shard_map(functools.partial(shards, sizes), mesh=mesh, in_specs=in_specs,
                         out_specs=out_specs, check_vma=False)
```

```python
import functools

import jax
import jax.numpy as jnp
from jax import lax
from jax.experimental import pallas as pl
from jax.experimental.pallas import tpu as pltpu
from jax.sharding import PartitionSpec as P

ITERS = 5
EPSILON = 1e-06
DIAGONAL = 6.0
FIRST_SHIFTS = (2.25, 8.25)
MESH = pl.DeviceIdType.MESH
AXES = ("slab", "py", "pz")
UNROLLED = 64
PLAN = (2, 3)


def times(coeff, columns):
    total = {}
    for k, c in coeff.items():
        for q, value in columns[k].items():
            term = c * value
            total[q] = total[q] + term if q in total else term
    return total


def dot(left, right):
    total = None
    for q, value in left.items():
        if q in right:
            term = value * right[q]
            total = term if total is None else total + term
    return 0.0 if total is None else total


def advance(j, steps, inner, shifts, taus, removed, betas):
    vectors = [{k: 1.0} for k in range(j + 1)]
    image_of = [{**removed[k], k + 1: betas[k]} for k in range(j)]
    for i in range(steps):
        column = {j + i + 1: 1.0, j + i: shifts[i]}
        if taus[i] is not None:
            column[j + i - 1] = taus[i]
        image_of.append(column)
    gram, lowered = {}, []
    for n in range(j, j + steps):
        for k in range(len(lowered), n + 1):
            lowered.append({
                q: dot(vectors[k], {b: inner[q, b] for b in vectors[k]})
                for q in range(n + 1)})
            for l in range(k + 1):
                gram[k, l] = gram[l, k] = dot(vectors[l], lowered[k])
        known = {n: shifts[n - j]}
        if n > j:
            known[n - 1] = betas[n - 1]
            rest = times(vectors[n], image_of)
            for k, y in known.items():
                for q, value in vectors[k].items():
                    rest[q] = rest[q] - y * value if q in rest else -y * value
        else:
            if taus[0] is not None:
                known[n - 1] = taus[0]
            rest = {n + 1: 1.0}
        rest_lowered = {
            q: dot(rest, {b: inner[q, b] for b in rest}) for q in range(n + 2)}
        along = {k: dot(vectors[k], rest_lowered) for k in range(n + 1)}
        first = {
            k: along[k] + dot(known, {l: gram[k, l] for l in known}) for k in range(n + 1)}
        excess = {k: first[k] - known[k] if k in known else first[k] for k in range(n + 1)}
        coeffs = {
            k: along[k] - dot(excess, {
                l: gram[k, l] - 1.0 if k == l else gram[k, l] for l in range(n + 1)})
            for k in range(n + 1)}
        square = dot(rest, rest_lowered)
        for k in range(n + 1):
            back = dot(coeffs, {l: gram[k, l] for l in range(n + 1)})
            square = square + coeffs[k] * (back - 2.0 * along[k])
        beta = jnp.sqrt(jnp.maximum(square, 0.0) + EPSILON)
        inverse = 1.0 / beta
        image = dict(rest)
        for k in range(n + 1):
            for q, value in vectors[k].items():
                term = coeffs[k] * value
                image[q] = image[q] - term if q in image else -term
        vectors.append({q: value * inverse for q, value in image.items()})
        removed.append({k: coeffs[k] + known[k] if k in known else coeffs[k] for k in coeffs})
        betas.append(beta)
    return vectors[j + 1:]


def basis_of(j, steps, removed, betas, start):
    if j == 0:
        return [start + shift for shift in FIRST_SHIFTS[:steps]], [None] * steps
    shift, beta = removed[j - 1][j - 1], betas[j - 1]
    return [shift] * steps, [beta] + [beta * beta] * (steps - 1)


def kernel(sizes, per_cell, x_ref, pot_ref, out_ref, tri_ref, work, ysend, zface, yface, xface,
           rz, ry, rx, slots, send_sem, recv_sem, stat_send, stat_recv):
    Z, Y, X = x_ref.shape
    S, A, B = sizes
    n = S * A * B
    slab, py, pz = (lax.axis_index(name) for name in AXES)
    me = (slab * A + py) * B + pz
    partner = lax.rem(slab + 1, S)

    def to_others(act):
        if n <= UNROLLED:
            slabs = [lax.rem(slab + i, S) for i in range(S)]
            pys = [lax.rem(py + i, A) for i in range(A)]
            pzs = [lax.rem(pz + i, B) for i in range(B)]
            far = sorted(
                ((i, j, k) for i in range(S) for j in range(A) for k in range(B)),
                key=lambda t: -(min(t[1], A - t[1]) + min(t[2], B - t[2])),
            )
            for i, j, k in far:
                if i or j or k:
                    act((slabs[i], pys[j], pzs[k]))
        else:
            def step(d, carry):
                t = lax.rem(me + d, n)
                act((t // (A * B), lax.rem(t // B, A), lax.rem(t, B)))
                return carry
            lax.fori_loop(1, n, step, 0)

    def halo_copies(p, zlo, zhi, block):
        def copy(src, dst, side, target):
            return pltpu.make_async_remote_copy(
                src_ref=src, dst_ref=dst, send_sem=send_sem.at[p, side],
                recv_sem=recv_sem.at[p, side], device_id=target, device_id_type=MESH)
        return (
            (pz < B - 1, pz > 0, copy(zhi, rz.at[p, 0], 0, (slab, py, pz + 1))),
            (pz > 0, pz < B - 1, copy(zlo, rz.at[p, 1], 1, (slab, py, pz - 1))),
            (py < A - 1, py > 0, copy(ysend.at[p, 1], ry.at[p, 0], 2, (slab, py + 1, pz))),
            (py > 0, py < A - 1, copy(ysend.at[p, 0], ry.at[p, 1], 3, (slab, py - 1, pz))),
            (None, None, copy(block, rx.at[p], 4, (partner, py, pz))),
        )

    def when(cond, act):
        if cond is None:
            act()
        else:
            pl.when(cond)(act)

    def exchange(p, zlo, zhi, block):
        copies = halo_copies(p, zlo, zhi, block)
        for sends, _, copy in copies:
            when(sends, copy.start)
        return copies

    def arrived(copies):
        for _, receives, copy in copies:
            when(receives, copy.wait_recv)

    def sent(copies):
        for sends, _, copy in copies:
            when(sends, copy.wait_send)

    def stat_copy(p, target):
        return pltpu.make_async_remote_copy(
            src_ref=slots.at[p, me], dst_ref=slots.at[p, me], send_sem=stat_send.at[p],
            recv_sem=stat_recv.at[p], device_id=target, device_id_type=MESH)

    def wait_all(p, sem):
        span = slots.at[p, pl.ds(0, n - 1)]
        pltpu.make_async_copy(span, span, sem).wait()

    lane = lax.broadcasted_iota(jnp.int32, (Y, X), 1)
    row = lax.broadcasted_iota(jnp.int32, (Y, X), 0)
    has_low = (slab > 0).astype(jnp.float32)
    has_high = (slab < S - 1).astype(jnp.float32)

    def stencil(z, own, zf, yf, xf):
        here = own(z)
        below = own(z - 1) if z > 0 else zf(0)
        above = own(z + 1) if z < Z - 1 else zf(1)
        ylow = jnp.where(row == 0, yf(0, z), pltpu.roll(here, 1, 0))
        yhigh = jnp.where(row == Y - 1, yf(1, z), pltpu.roll(here, Y - 1, 0))
        side = xf(z)
        xlow = pltpu.roll(jnp.where(lane == X - 1, side * has_low, here), 1, 1)
        xhigh = pltpu.roll(jnp.where(lane == 0, side * has_high, here), X - 1, 1)
        return (above + below) + (yhigh + ylow) + (xhigh + xlow)

    def fold(value):
        return jnp.sum(value.reshape(Y // 8, 8, X), axis=0)

    def share(p, sums):
        rows = [jnp.sum(v, axis=0, keepdims=True) for v in sums]
        height = -(-len(rows) // 8) * 8
        rows = rows + [jnp.zeros((1, X), jnp.float32)] * (height - len(rows))
        totals = jnp.sum(jnp.concatenate(rows, axis=0), axis=1, keepdims=True)
        at = lax.broadcasted_iota(jnp.int32, (height, X), 0)
        lanes = lax.broadcasted_iota(jnp.int32, (height, X), 1)
        slots[p, me] = jnp.sum(jnp.where(at == lanes, totals, 0.0), axis=0, keepdims=True)
        to_others(lambda target: stat_copy(p, target).start())

    def gathered(p, count):
        wait_all(p, stat_recv.at[p])
        total = jnp.sum(slots[p], axis=0) * per_cell
        return [jnp.broadcast_to(total[:, s:s + 1], (1, X)) for s in range(count)]

    for p in range(ITERS):
        for side, missing in ((0, pz == 0), (1, pz == B - 1)):
            @pl.when(missing)
            def _(p=p, side=side):
                rz[p, side] = jnp.zeros((Y, X), jnp.float32)
        for side, missing in ((0, py == 0), (1, py == A - 1)):
            @pl.when(missing)
            def _(p=p, side=side):
                ry[p, side] = jnp.zeros((Z, X), jnp.float32)
    for z in range(Z):
        ysend[0, 0, z:z + 1] = x_ref[z, 0:1, :]
        ysend[0, 1, z:z + 1] = x_ref[z, Y - 1:Y, :]

    barrier = pltpu.get_barrier_semaphore()
    to_others(lambda t: pl.semaphore_signal(barrier, inc=1, device_id=t, device_id_type=MESH))
    pl.semaphore_wait(barrier, n - 1)

    pending = [exchange(0, x_ref.at[0], x_ref.at[Z - 1], x_ref)]

    def vector(k):
        if k == 0 and base == 0:
            return (lambda z: x_ref[z]), *faces(0)
        return ((lambda z: out_ref[k, z]), (lambda f: zface[k, f]),
                (lambda f, z: yface[k, f, z:z + 1, :]), (lambda z: xface[k, z]),
                (lambda f: yface[k, f]))

    def faces(e):
        return ((lambda f: rz[e, f]), (lambda f, z: ry[e, f, z:z + 1, :]), (lambda z: rx[e, z]),
                (lambda f: ry[e, f]))

    def powered(e):
        return (lambda z: work[e - 1, z]), *faces(e)

    removed, betas, inner, fresh = [], [], {}, range(1)
    start = jnp.zeros((1, X), jnp.float32)
    base, applied = 0, 0
    for phase, steps in enumerate(PLAN):
        last = base + steps == ITERS
        shifts, taus = basis_of(base, steps, removed, betas, start)
        held = [vector(k) for k in range(base + 1)]
        pairs, sums = [], []

        def measure(n, held=held, pairs=pairs, sums=sums):
            totals = [jnp.zeros((8, X), jnp.float32)] * (n + 1)
            for z in range(Z):
                newest = held[n][0](z)
                for k in range(n + 1):
                    totals[k] = totals[k] + fold(held[k][0](z) * newest)
            pairs.extend((k, n) for k in range(n + 1))
            sums.extend(totals)

        if phase == 0:
            for v in fresh:
                measure(v)
            arrived(pending[0])
        for i in range(steps):
            own, zf, yf, xf, _ = held[base + i]
            applied += 1
            ends = applied == ITERS
            for z in range(Z):
                image = (((DIAGONAL - shifts[i]) + pot_ref[z]) * own(z)
                         - stencil(z, own, zf, yf, xf))
                if taus[i] is not None:
                    image = image - taus[i] * held[base + i - 1][0](z)
                work[applied - 1, z] = image
                if not ends:
                    ysend[applied, 0, z:z + 1] = image[0:1]
                    ysend[applied, 1, z:z + 1] = image[Y - 1:Y]
            held.append(powered(applied))
            if not ends:
                pending.append(exchange(applied, work.at[applied - 1, 0],
                                        work.at[applied - 1, Z - 1], work.at[applied - 1]))
            if i == 0 and phase > 0:
                for v in fresh:
                    measure(v)
            measure(base + i + 1)
            if i < steps - 1:
                arrived(pending[applied])
        share(phase, sums)
        stats = gathered(phase, len(sums))
        if phase == 0:
            scale = 1.0 / jnp.sqrt(stats[0] + EPSILON)
            stats = [s * scale * scale for s in stats]
        for (k, l), value in zip(pairs, stats):
            inner[k, l] = inner[l, k] = value
        found = advance(base, steps, inner, shifts, taus, removed, betas)
        for v in range(base, base + steps):
            tri_ref[0:1, v:v + 1] = removed[v][v][:, 0:1]
            tri_ref[1:2, v:v + 1] = betas[v][:, 0:1]
        if phase == 0:
            found = [{q: t * scale for q, t in coords.items()} for coords in found]
        if not last:
            arrived(pending[applied])

        def fill(get, put, only_last):
            columns = [get(held[q]) for q in range(base + steps + 1)]
            if phase == 0 and not (only_last and len(PLAN) == 2):
                put(0, columns[0] * scale)
            for i, coords in enumerate(found):
                if only_last and phase == len(PLAN) - 2 and i < steps - 1:
                    continue
                total = None
                for q in sorted(coords, reverse=True):
                    term = coords[q] * columns[q]
                    total = term if total is None else total + term
                put(base + 1 + i, total)

        def putter(ref, *index):
            def put(k, value):
                ref[(k,) + index] = value
            return put

        for z in range(Z):
            fill(lambda h: h[0](z), putter(out_ref, z), False)
            if not last:
                fill(lambda h: h[3](z), putter(xface, z), True)
        if not last:
            for f in range(2):
                fill(lambda h: h[1](f), putter(zface, f), True)
                fill(lambda h: h[4](f), putter(yface, f), True)
        inner = {pair: value for pair, value in inner.items() if max(pair) <= base}
        fresh = range(base + 1, base + steps + 1)
        base += steps

    for copies in pending:
        sent(copies)
    for p in range(len(PLAN)):
        wait_all(p, stat_send.at[p])


def shards(sizes, start_vector, potential):
    Z, Y, X = start_vector.shape
    n = sizes[0] * sizes[1] * sizes[2]
    f32 = jnp.float32
    vmem = pl.BlockSpec(memory_space=pltpu.VMEM)
    return tuple(pl.pallas_call(
        functools.partial(kernel, sizes, 1.0 / (start_vector.size * n)),
        out_shape=(jax.ShapeDtypeStruct((ITERS + 1, Z, Y, X), f32),
                   jax.ShapeDtypeStruct((2, ITERS), f32)),
        in_specs=[vmem, vmem],
        out_specs=(vmem, vmem),
        scratch_shapes=[
            pltpu.VMEM((ITERS, Z, Y, X), f32),
            pltpu.VMEM((ITERS, 2, Z, X), f32),
            pltpu.VMEM((ITERS, 2, Y, X), f32),
            pltpu.VMEM((ITERS, 2, Z, X), f32),
            pltpu.VMEM((ITERS, Z, Y, X), f32),
            pltpu.VMEM((ITERS, 2, Y, X), f32),
            pltpu.VMEM((ITERS, 2, Z, X), f32),
            pltpu.VMEM((ITERS, Z, Y, X), f32),
            pltpu.VMEM((ITERS, n, 1, X), f32),
            pltpu.SemaphoreType.DMA((ITERS, 5)),
            pltpu.SemaphoreType.DMA((ITERS, 5)),
            pltpu.SemaphoreType.DMA((ITERS,)),
            pltpu.SemaphoreType.DMA((ITERS,)),
        ],
        compiler_params=pltpu.CompilerParams(collective_id=0, has_side_effects=True),
    )(start_vector, potential))


def solution(mesh):
    sizes = tuple(mesh.shape[name] for name in AXES)
    in_specs = (P("pz", "py", "slab"), P("pz", "py", "slab"))
    out_specs = (P(None, "pz", "py", "slab"), P())
    return jax.shard_map(functools.partial(shards, sizes), mesh=mesh, in_specs=in_specs,
                         out_specs=out_specs, check_vma=False)
```

```python
import functools

import jax
import jax.numpy as jnp
from jax import lax
from jax.experimental import pallas as pl
from jax.experimental.pallas import tpu as pltpu
from jax.sharding import PartitionSpec as P

ITERS = 5
EPSILON = 1e-06
DIAGONAL = 6.0
FIRST_SHIFTS = (3.5, 10.0)
MESH = pl.DeviceIdType.MESH
AXES = ("slab", "py", "pz")
UNROLLED = 64
PLAN = (2, 3)


def times(coeff, columns):
    total = {}
    for k, c in coeff.items():
        for q, value in columns[k].items():
            term = c * value
            total[q] = total[q] + term if q in total else term
    return total


def dot(left, right):
    total = None
    for q, value in left.items():
        if q in right:
            term = value * right[q]
            total = term if total is None else total + term
    return 0.0 if total is None else total


def advance(j, steps, inner, shifts, taus, removed, betas):
    vectors = [{k: 1.0} for k in range(j + 1)]
    image_of = [{**removed[k], k + 1: betas[k]} for k in range(j)]
    for i in range(steps):
        column = {j + i + 1: 1.0, j + i: shifts[i]}
        if taus[i] is not None:
            column[j + i - 1] = taus[i]
        image_of.append(column)
    gram, lowered = {}, []
    for n in range(j, j + steps):
        for k in range(len(lowered), n + 1):
            lowered.append({
                q: dot(vectors[k], {b: inner[q, b] for b in vectors[k]})
                for q in range(n + 1)})
            for l in range(k + 1):
                gram[k, l] = gram[l, k] = dot(vectors[l], lowered[k])
        known = {n: shifts[n - j]}
        if n > j:
            known[n - 1] = betas[n - 1]
            rest = times(vectors[n], image_of)
            for k, y in known.items():
                for q, value in vectors[k].items():
                    rest[q] = rest[q] - y * value if q in rest else -y * value
        else:
            if taus[0] is not None:
                known[n - 1] = taus[0]
            rest = {n + 1: 1.0}
        rest_lowered = {
            q: dot(rest, {b: inner[q, b] for b in rest}) for q in range(n + 2)}
        along = {k: dot(vectors[k], rest_lowered) for k in range(n + 1)}
        first = {
            k: along[k] + dot(known, {l: gram[k, l] for l in known}) for k in range(n + 1)}
        excess = {k: first[k] - known[k] if k in known else first[k] for k in range(n + 1)}
        coeffs = {
            k: along[k] - dot(excess, {
                l: gram[k, l] - 1.0 if k == l else gram[k, l] for l in range(n + 1)})
            for k in range(n + 1)}
        square = dot(rest, rest_lowered)
        for k in range(n + 1):
            back = dot(coeffs, {l: gram[k, l] for l in range(n + 1)})
            square = square + coeffs[k] * (back - 2.0 * along[k])
        beta = jnp.sqrt(jnp.maximum(square, 0.0) + EPSILON)
        inverse = 1.0 / beta
        image = dict(rest)
        for k in range(n + 1):
            for q, value in vectors[k].items():
                term = coeffs[k] * value
                image[q] = image[q] - term if q in image else -term
        vectors.append({q: value * inverse for q, value in image.items()})
        removed.append({k: coeffs[k] + known[k] if k in known else coeffs[k] for k in coeffs})
        betas.append(beta)
    return vectors[j + 1:]


def basis_of(j, steps, removed, betas, start):
    if j == 0:
        return [start + shift for shift in FIRST_SHIFTS[:steps]], [None] * steps
    shift, beta = removed[j - 1][j - 1], betas[j - 1]
    return [shift] * steps, [beta] + [beta * beta] * (steps - 1)


def kernel(sizes, per_cell, x_ref, pot_ref, out_ref, tri_ref, work, ysend, zface, yface, xface,
           rz, ry, rx, slots, send_sem, recv_sem, stat_send, stat_recv):
    Z, Y, X = x_ref.shape
    S, A, B = sizes
    n = S * A * B
    slab, py, pz = (lax.axis_index(name) for name in AXES)
    me = (slab * A + py) * B + pz
    partner = lax.rem(slab + 1, S)

    def to_others(act):
        if n <= UNROLLED:
            slabs = [lax.rem(slab + i, S) for i in range(S)]
            pys = [lax.rem(py + i, A) for i in range(A)]
            pzs = [lax.rem(pz + i, B) for i in range(B)]
            far = sorted(
                ((i, j, k) for i in range(S) for j in range(A) for k in range(B)),
                key=lambda t: -(min(t[1], A - t[1]) + min(t[2], B - t[2])),
            )
            for i, j, k in far:
                if i or j or k:
                    act((slabs[i], pys[j], pzs[k]))
        else:
            def step(d, carry):
                t = lax.rem(me + d, n)
                act((t // (A * B), lax.rem(t // B, A), lax.rem(t, B)))
                return carry
            lax.fori_loop(1, n, step, 0)

    def halo_copies(p, zlo, zhi, block):
        def copy(src, dst, side, target):
            return pltpu.make_async_remote_copy(
                src_ref=src, dst_ref=dst, send_sem=send_sem.at[p, side],
                recv_sem=recv_sem.at[p, side], device_id=target, device_id_type=MESH)
        return (
            (pz < B - 1, pz > 0, copy(zhi, rz.at[p, 0], 0, (slab, py, pz + 1))),
            (pz > 0, pz < B - 1, copy(zlo, rz.at[p, 1], 1, (slab, py, pz - 1))),
            (py < A - 1, py > 0, copy(ysend.at[p, 1], ry.at[p, 0], 2, (slab, py + 1, pz))),
            (py > 0, py < A - 1, copy(ysend.at[p, 0], ry.at[p, 1], 3, (slab, py - 1, pz))),
            (None, None, copy(block, rx.at[p], 4, (partner, py, pz))),
        )

    def when(cond, act):
        if cond is None:
            act()
        else:
            pl.when(cond)(act)

    def exchange(p, zlo, zhi, block):
        copies = halo_copies(p, zlo, zhi, block)
        for sends, _, copy in copies:
            when(sends, copy.start)
        return copies

    def arrived(copies):
        for _, receives, copy in copies:
            when(receives, copy.wait_recv)

    def sent(copies):
        for sends, _, copy in copies:
            when(sends, copy.wait_send)

    def stat_copy(p, target):
        return pltpu.make_async_remote_copy(
            src_ref=slots.at[p, me], dst_ref=slots.at[p, me], send_sem=stat_send.at[p],
            recv_sem=stat_recv.at[p], device_id=target, device_id_type=MESH)

    def wait_all(p, sem):
        span = slots.at[p, pl.ds(0, n - 1)]
        pltpu.make_async_copy(span, span, sem).wait()

    lane = lax.broadcasted_iota(jnp.int32, (Y, X), 1)
    row = lax.broadcasted_iota(jnp.int32, (Y, X), 0)
    has_low = (slab > 0).astype(jnp.float32)
    has_high = (slab < S - 1).astype(jnp.float32)

    def stencil(z, own, zf, yf, xf):
        here = own(z)
        below = own(z - 1) if z > 0 else zf(0)
        above = own(z + 1) if z < Z - 1 else zf(1)
        ylow = jnp.where(row == 0, yf(0, z), pltpu.roll(here, 1, 0))
        yhigh = jnp.where(row == Y - 1, yf(1, z), pltpu.roll(here, Y - 1, 0))
        side = xf(z)
        xlow = pltpu.roll(jnp.where(lane == X - 1, side * has_low, here), 1, 1)
        xhigh = pltpu.roll(jnp.where(lane == 0, side * has_high, here), X - 1, 1)
        return (above + below) + (yhigh + ylow) + (xhigh + xlow)

    def fold(value):
        return jnp.sum(value.reshape(Y // 8, 8, X), axis=0)

    def share(p, sums):
        rows = [jnp.sum(v, axis=0, keepdims=True) for v in sums]
        height = -(-len(rows) // 8) * 8
        rows = rows + [jnp.zeros((1, X), jnp.float32)] * (height - len(rows))
        totals = jnp.sum(jnp.concatenate(rows, axis=0), axis=1, keepdims=True)
        at = lax.broadcasted_iota(jnp.int32, (height, X), 0)
        lanes = lax.broadcasted_iota(jnp.int32, (height, X), 1)
        slots[p, me] = jnp.sum(jnp.where(at == lanes, totals, 0.0), axis=0, keepdims=True)
        to_others(lambda target: stat_copy(p, target).start())

    def gathered(p, count):
        wait_all(p, stat_recv.at[p])
        total = jnp.sum(slots[p], axis=0) * per_cell
        return [jnp.broadcast_to(total[:, s:s + 1], (1, X)) for s in range(count)]

    for p in range(ITERS):
        for side, missing in ((0, pz == 0), (1, pz == B - 1)):
            @pl.when(missing)
            def _(p=p, side=side):
                rz[p, side] = jnp.zeros((Y, X), jnp.float32)
        for side, missing in ((0, py == 0), (1, py == A - 1)):
            @pl.when(missing)
            def _(p=p, side=side):
                ry[p, side] = jnp.zeros((Z, X), jnp.float32)
    for z in range(Z):
        ysend[0, 0, z:z + 1] = x_ref[z, 0:1, :]
        ysend[0, 1, z:z + 1] = x_ref[z, Y - 1:Y, :]

    barrier = pltpu.get_barrier_semaphore()
    to_others(lambda t: pl.semaphore_signal(barrier, inc=1, device_id=t, device_id_type=MESH))
    pl.semaphore_wait(barrier, n - 1)

    pending = [exchange(0, x_ref.at[0], x_ref.at[Z - 1], x_ref)]

    def vector(k):
        if k == 0 and base == 0:
            return (lambda z: x_ref[z]), *faces(0)
        return ((lambda z: out_ref[k, z]), (lambda f: zface[k, f]),
                (lambda f, z: yface[k, f, z:z + 1, :]), (lambda z: xface[k, z]),
                (lambda f: yface[k, f]))

    def faces(e):
        return ((lambda f: rz[e, f]), (lambda f, z: ry[e, f, z:z + 1, :]), (lambda z: rx[e, z]),
                (lambda f: ry[e, f]))

    def powered(e):
        return (lambda z: work[e - 1, z]), *faces(e)

    removed, betas, inner, fresh = [], [], {}, range(1)
    start = jnp.zeros((1, X), jnp.float32)
    base, applied = 0, 0
    for phase, steps in enumerate(PLAN):
        last = base + steps == ITERS
        shifts, taus = basis_of(base, steps, removed, betas, start)
        held = [vector(k) for k in range(base + 1)]
        pairs, sums = [], []

        def measure(n, held=held, pairs=pairs, sums=sums):
            totals = [jnp.zeros((8, X), jnp.float32)] * (n + 1)
            for z in range(Z):
                newest = held[n][0](z)
                for k in range(n + 1):
                    totals[k] = totals[k] + fold(held[k][0](z) * newest)
            pairs.extend((k, n) for k in range(n + 1))
            sums.extend(totals)

        if phase == 0:
            for v in fresh:
                measure(v)
            arrived(pending[0])
        for i in range(steps):
            own, zf, yf, xf, _ = held[base + i]
            applied += 1
            ends = applied == ITERS
            for z in range(Z):
                image = (((DIAGONAL - shifts[i]) + pot_ref[z]) * own(z)
                         - stencil(z, own, zf, yf, xf))
                if taus[i] is not None:
                    image = image - taus[i] * held[base + i - 1][0](z)
                work[applied - 1, z] = image
                if not ends:
                    ysend[applied, 0, z:z + 1] = image[0:1]
                    ysend[applied, 1, z:z + 1] = image[Y - 1:Y]
            held.append(powered(applied))
            if not ends:
                pending.append(exchange(applied, work.at[applied - 1, 0],
                                        work.at[applied - 1, Z - 1], work.at[applied - 1]))
            if i == 0 and phase > 0:
                for v in fresh:
                    measure(v)
            measure(base + i + 1)
            if i < steps - 1:
                arrived(pending[applied])
        share(phase, sums)
        stats = gathered(phase, len(sums))
        if phase == 0:
            scale = 1.0 / jnp.sqrt(stats[0] + EPSILON)
            stats = [s * scale * scale for s in stats]
        for (k, l), value in zip(pairs, stats):
            inner[k, l] = inner[l, k] = value
        found = advance(base, steps, inner, shifts, taus, removed, betas)
        for v in range(base, base + steps):
            tri_ref[0:1, v:v + 1] = removed[v][v][:, 0:1]
            tri_ref[1:2, v:v + 1] = betas[v][:, 0:1]
        if phase == 0:
            found = [{q: t * scale for q, t in coords.items()} for coords in found]
        if not last:
            arrived(pending[applied])

        def fill(get, put, only_last):
            columns = [get(held[q]) for q in range(base + steps + 1)]
            if phase == 0 and not (only_last and len(PLAN) == 2):
                put(0, columns[0] * scale)
            for i, coords in enumerate(found):
                if only_last and phase == len(PLAN) - 2 and i < steps - 1:
                    continue
                total = None
                for q in sorted(coords, reverse=True):
                    term = coords[q] * columns[q]
                    total = term if total is None else total + term
                put(base + 1 + i, total)

        def putter(ref, *index):
            def put(k, value):
                ref[(k,) + index] = value
            return put

        for z in range(Z):
            fill(lambda h: h[0](z), putter(out_ref, z), False)
            if not last:
                fill(lambda h: h[3](z), putter(xface, z), True)
        if not last:
            for f in range(2):
                fill(lambda h: h[1](f), putter(zface, f), True)
                fill(lambda h: h[4](f), putter(yface, f), True)
        inner = {pair: value for pair, value in inner.items() if max(pair) <= base}
        fresh = range(base + 1, base + steps + 1)
        base += steps

    for copies in pending:
        sent(copies)
    for p in range(len(PLAN)):
        wait_all(p, stat_send.at[p])


def shards(sizes, start_vector, potential):
    Z, Y, X = start_vector.shape
    n = sizes[0] * sizes[1] * sizes[2]
    f32 = jnp.float32
    vmem = pl.BlockSpec(memory_space=pltpu.VMEM)
    return tuple(pl.pallas_call(
        functools.partial(kernel, sizes, 1.0 / (start_vector.size * n)),
        out_shape=(jax.ShapeDtypeStruct((ITERS + 1, Z, Y, X), f32),
                   jax.ShapeDtypeStruct((2, ITERS), f32)),
        in_specs=[vmem, vmem],
        out_specs=(vmem, vmem),
        scratch_shapes=[
            pltpu.VMEM((ITERS, Z, Y, X), f32),
            pltpu.VMEM((ITERS, 2, Z, X), f32),
            pltpu.VMEM((ITERS, 2, Y, X), f32),
            pltpu.VMEM((ITERS, 2, Z, X), f32),
            pltpu.VMEM((ITERS, Z, Y, X), f32),
            pltpu.VMEM((ITERS, 2, Y, X), f32),
            pltpu.VMEM((ITERS, 2, Z, X), f32),
            pltpu.VMEM((ITERS, Z, Y, X), f32),
            pltpu.VMEM((ITERS, n, 1, X), f32),
            pltpu.SemaphoreType.DMA((ITERS, 5)),
            pltpu.SemaphoreType.DMA((ITERS, 5)),
            pltpu.SemaphoreType.DMA((ITERS,)),
            pltpu.SemaphoreType.DMA((ITERS,)),
        ],
        compiler_params=pltpu.CompilerParams(collective_id=0, has_side_effects=True),
    )(start_vector, potential))


def solution(mesh):
    sizes = tuple(mesh.shape[name] for name in AXES)
    in_specs = (P("pz", "py", "slab"), P("pz", "py", "slab"))
    out_specs = (P(None, "pz", "py", "slab"), P())
    return jax.shard_map(functools.partial(shards, sizes), mesh=mesh, in_specs=in_specs,
                         out_specs=out_specs, check_vma=False)
```

```python
import functools

import jax
import jax.numpy as jnp
from jax import lax
from jax.experimental import pallas as pl
from jax.experimental.pallas import tpu as pltpu
from jax.sharding import PartitionSpec as P

ITERS = 5
EPSILON = 1e-06
DIAGONAL = 6.0
FIRST_SHIFTS = (3.5, 10.0)
MESH = pl.DeviceIdType.MESH
AXES = ("slab", "py", "pz")
UNROLLED = 64
PLAN = (2, 3)


def times(coeff, columns):
    total = {}
    for k, c in coeff.items():
        for q, value in columns[k].items():
            term = c * value
            total[q] = total[q] + term if q in total else term
    return total


def dot(left, right):
    total = None
    for q, value in left.items():
        if q in right:
            term = value * right[q]
            total = term if total is None else total + term
    return 0.0 if total is None else total


def advance(j, steps, inner, shifts, taus, removed, betas):
    vectors = [{k: 1.0} for k in range(j + 1)]
    image_of = [{**removed[k], k + 1: betas[k]} for k in range(j)]
    for i in range(steps):
        column = {j + i + 1: 1.0, j + i: shifts[i]}
        if taus[i] is not None:
            column[j + i - 1] = taus[i]
        image_of.append(column)
    gram, lowered = {}, []
    for n in range(j, j + steps):
        for k in range(len(lowered), n + 1):
            lowered.append({
                q: dot(vectors[k], {b: inner[q, b] for b in vectors[k]})
                for q in range(n + 1)})
            for l in range(k + 1):
                gram[k, l] = gram[l, k] = dot(vectors[l], lowered[k])
        known = {n: shifts[n - j]}
        if n > j:
            known[n - 1] = betas[n - 1]
            rest = times(vectors[n], image_of)
            for k, y in known.items():
                for q, value in vectors[k].items():
                    rest[q] = rest[q] - y * value if q in rest else -y * value
        else:
            if taus[0] is not None:
                known[n - 1] = taus[0]
            rest = {n + 1: 1.0}
        rest_lowered = {
            q: dot(rest, {b: inner[q, b] for b in rest}) for q in range(n + 2)}
        along = {k: dot(vectors[k], rest_lowered) for k in range(n + 1)}
        first = {
            k: along[k] + dot(known, {l: gram[k, l] for l in known}) for k in range(n + 1)}
        excess = {k: first[k] - known[k] if k in known else first[k] for k in range(n + 1)}
        coeffs = {
            k: along[k] - dot(excess, {
                l: gram[k, l] - 1.0 if k == l else gram[k, l] for l in range(n + 1)})
            for k in range(n + 1)}
        square = dot(rest, rest_lowered)
        for k in range(n + 1):
            back = dot(coeffs, {l: gram[k, l] for l in range(n + 1)})
            square = square + coeffs[k] * (back - 2.0 * along[k])
        beta = jnp.sqrt(jnp.maximum(square, 0.0) + EPSILON)
        inverse = 1.0 / beta
        image = dict(rest)
        for k in range(n + 1):
            for q, value in vectors[k].items():
                term = coeffs[k] * value
                image[q] = image[q] - term if q in image else -term
        vectors.append({q: value * inverse for q, value in image.items()})
        removed.append({k: coeffs[k] + known[k] if k in known else coeffs[k] for k in coeffs})
        betas.append(beta)
    return vectors[j + 1:]


def basis_of(j, steps, removed, betas, start):
    if j == 0:
        return [start + shift for shift in FIRST_SHIFTS[:steps]], [None] * steps
    shift, beta = removed[j - 1][j - 1], betas[j - 1]
    return [shift] * steps, [beta] + [beta * beta] * (steps - 1)


def kernel(sizes, per_cell, x_ref, pot_ref, out_ref, tri_ref, work, ysend, zface, yface, xface,
           rz, ry, rx, slots, send_sem, recv_sem, stat_send, stat_recv):
    Z, Y, X = x_ref.shape
    S, A, B = sizes
    n = S * A * B
    slab, py, pz = (lax.axis_index(name) for name in AXES)
    me = (slab * A + py) * B + pz
    partner = lax.rem(slab + 1, S)

    def to_others(act):
        if n <= UNROLLED:
            slabs = [lax.rem(slab + i, S) for i in range(S)]
            pys = [lax.rem(py + i, A) for i in range(A)]
            pzs = [lax.rem(pz + i, B) for i in range(B)]
            far = sorted(
                ((i, j, k) for i in range(S) for j in range(A) for k in range(B)),
                key=lambda t: -(min(t[1], A - t[1]) + min(t[2], B - t[2])),
            )
            for i, j, k in far:
                if i or j or k:
                    act((slabs[i], pys[j], pzs[k]))
        else:
            def step(d, carry):
                t = lax.rem(me + d, n)
                act((t // (A * B), lax.rem(t // B, A), lax.rem(t, B)))
                return carry
            lax.fori_loop(1, n, step, 0)

    def halo_copies(p, zlo, zhi, block):
        def copy(src, dst, side, target):
            return pltpu.make_async_remote_copy(
                src_ref=src, dst_ref=dst, send_sem=send_sem.at[p, side],
                recv_sem=recv_sem.at[p, side], device_id=target, device_id_type=MESH)
        return (
            (pz < B - 1, pz > 0, copy(zhi, rz.at[p, 0], 0, (slab, py, pz + 1))),
            (pz > 0, pz < B - 1, copy(zlo, rz.at[p, 1], 1, (slab, py, pz - 1))),
            (py < A - 1, py > 0, copy(ysend.at[p, 1], ry.at[p, 0], 2, (slab, py + 1, pz))),
            (py > 0, py < A - 1, copy(ysend.at[p, 0], ry.at[p, 1], 3, (slab, py - 1, pz))),
            (None, None, copy(block, rx.at[p], 4, (partner, py, pz))),
        )

    def when(cond, act):
        if cond is None:
            act()
        else:
            pl.when(cond)(act)

    def exchange(p, zlo, zhi, block):
        copies = halo_copies(p, zlo, zhi, block)
        for sends, _, copy in copies:
            when(sends, copy.start)
        return copies

    def arrived(copies):
        for _, receives, copy in copies:
            when(receives, copy.wait_recv)

    def sent(copies):
        for sends, _, copy in copies:
            when(sends, copy.wait_send)

    def stat_copy(p, target):
        return pltpu.make_async_remote_copy(
            src_ref=slots.at[p, me], dst_ref=slots.at[p, me], send_sem=stat_send.at[p],
            recv_sem=stat_recv.at[p], device_id=target, device_id_type=MESH)

    def wait_all(p, sem):
        span = slots.at[p, pl.ds(0, n - 1)]
        pltpu.make_async_copy(span, span, sem).wait()

    lane = lax.broadcasted_iota(jnp.int32, (Y, X), 1)
    row = lax.broadcasted_iota(jnp.int32, (Y, X), 0)
    has_low = (slab > 0).astype(jnp.float32)
    has_high = (slab < S - 1).astype(jnp.float32)

    def stencil(z, own, zf, yf, xf):
        here = own(z)
        below = own(z - 1) if z > 0 else zf(0)
        above = own(z + 1) if z < Z - 1 else zf(1)
        ylow = jnp.where(row == 0, yf(0, z), pltpu.roll(here, 1, 0))
        yhigh = jnp.where(row == Y - 1, yf(1, z), pltpu.roll(here, Y - 1, 0))
        side = xf(z)
        xlow = pltpu.roll(jnp.where(lane == X - 1, side * has_low, here), 1, 1)
        xhigh = pltpu.roll(jnp.where(lane == 0, side * has_high, here), X - 1, 1)
        return (above + below) + (yhigh + ylow) + (xhigh + xlow)

    def fold(value):
        return jnp.sum(value.reshape(Y // 8, 8, X), axis=0)

    def share(p, sums):
        rows = [jnp.sum(v, axis=0, keepdims=True) for v in sums]
        height = -(-len(rows) // 8) * 8
        rows = rows + [jnp.zeros((1, X), jnp.float32)] * (height - len(rows))
        totals = jnp.sum(jnp.concatenate(rows, axis=0), axis=1, keepdims=True)
        at = lax.broadcasted_iota(jnp.int32, (height, X), 0)
        lanes = lax.broadcasted_iota(jnp.int32, (height, X), 1)
        slots[p, me] = jnp.sum(jnp.where(at == lanes, totals, 0.0), axis=0, keepdims=True)
        to_others(lambda target: stat_copy(p, target).start())

    def gathered(p, count):
        wait_all(p, stat_recv.at[p])
        total = jnp.sum(slots[p], axis=0) * per_cell
        return [jnp.broadcast_to(total[:, s:s + 1], (1, X)) for s in range(count)]

    for p in range(ITERS):
        for side, missing in ((0, pz == 0), (1, pz == B - 1)):
            @pl.when(missing)
            def _(p=p, side=side):
                rz[p, side] = jnp.zeros((Y, X), jnp.float32)
        for side, missing in ((0, py == 0), (1, py == A - 1)):
            @pl.when(missing)
            def _(p=p, side=side):
                ry[p, side] = jnp.zeros((Z, X), jnp.float32)
    for z in range(Z):
        ysend[0, 0, z:z + 1] = x_ref[z, 0:1, :]
        ysend[0, 1, z:z + 1] = x_ref[z, Y - 1:Y, :]

    barrier = pltpu.get_barrier_semaphore()
    to_others(lambda t: pl.semaphore_signal(barrier, inc=1, device_id=t, device_id_type=MESH))
    pl.semaphore_wait(barrier, n - 1)

    pending = [exchange(0, x_ref.at[0], x_ref.at[Z - 1], x_ref)]

    def vector(k):
        if k == 0 and base == 0:
            return (lambda z: x_ref[z]), *faces(0)
        return ((lambda z: out_ref[k, z]), (lambda f: zface[k, f]),
                (lambda f, z: yface[k, f, z:z + 1, :]), (lambda z: xface[k, z]),
                (lambda f: yface[k, f]))

    def faces(e):
        return ((lambda f: rz[e, f]), (lambda f, z: ry[e, f, z:z + 1, :]), (lambda z: rx[e, z]),
                (lambda f: ry[e, f]))

    def powered(e):
        return (lambda z: work[e - 1, z]), *faces(e)

    removed, betas, inner, fresh = [], [], {}, range(1)
    start = jnp.zeros((1, X), jnp.float32)
    base, applied = 0, 0
    for phase, steps in enumerate(PLAN):
        last = base + steps == ITERS
        shifts, taus = basis_of(base, steps, removed, betas, start)
        held = [vector(k) for k in range(base + 1)]
        pairs, sums = [], []

        def measure(n, held=held, pairs=pairs, sums=sums):
            totals = [jnp.zeros((8, X), jnp.float32)] * (n + 1)
            for z in range(Z):
                newest = held[n][0](z)
                for k in range(n + 1):
                    totals[k] = totals[k] + fold(held[k][0](z) * newest)
            pairs.extend((k, n) for k in range(n + 1))
            sums.extend(totals)

        if phase == 0:
            for v in fresh:
                measure(v)
            arrived(pending[0])
        for i in range(steps):
            own, zf, yf, xf, _ = held[base + i]
            applied += 1
            ends = applied == ITERS
            for z in range(Z):
                image = (((DIAGONAL - shifts[i]) + pot_ref[z]) * own(z)
                         - stencil(z, own, zf, yf, xf))
                if taus[i] is not None:
                    image = image - taus[i] * held[base + i - 1][0](z)
                work[applied - 1, z] = image
                if not ends:
                    ysend[applied, 0, z:z + 1] = image[0:1]
                    ysend[applied, 1, z:z + 1] = image[Y - 1:Y]
            held.append(powered(applied))
            if not ends:
                pending.append(exchange(applied, work.at[applied - 1, 0],
                                        work.at[applied - 1, Z - 1], work.at[applied - 1]))
            if i == 0 and phase > 0:
                for v in fresh:
                    measure(v)
            measure(base + i + 1)
            if i < steps - 1:
                arrived(pending[applied])
        share(phase, sums)
        stats = gathered(phase, len(sums))
        if phase == 0:
            scale = 1.0 / jnp.sqrt(stats[0] + EPSILON)
            stats = [s * scale * scale for s in stats]
        for (k, l), value in zip(pairs, stats):
            inner[k, l] = inner[l, k] = value
        found = advance(base, steps, inner, shifts, taus, removed, betas)
        for v in range(base, base + steps):
            tri_ref[0:1, v:v + 1] = removed[v][v][:, 0:1]
            tri_ref[1:2, v:v + 1] = betas[v][:, 0:1]
        if phase == 0:
            found = [{q: t * scale for q, t in coords.items()} for coords in found]
        if not last:
            arrived(pending[applied])

        def fill(get, put, only_last):
            columns = [get(held[q]) for q in range(base + steps + 1)]
            if phase == 0 and not (only_last and len(PLAN) == 2):
                put(0, columns[0] * scale)
            for i, coords in enumerate(found):
                if only_last and phase == len(PLAN) - 2 and i < steps - 1:
                    continue
                total = None
                for q in sorted(coords, reverse=True):
                    term = coords[q] * columns[q]
                    total = term if total is None else total + term
                put(base + 1 + i, total)

        def putter(ref, *index):
            def put(k, value):
                ref[(k,) + index] = value
            return put

        for z in range(Z):
            fill(lambda h: h[0](z), putter(out_ref, z), False)
            if not last:
                fill(lambda h: h[3](z), putter(xface, z), True)
        if not last:
            for f in range(2):
                fill(lambda h: h[1](f), putter(zface, f), True)
                fill(lambda h: h[4](f), putter(yface, f), True)
        inner = {pair: value for pair, value in inner.items() if max(pair) <= base}
        fresh = range(base + 1, base + steps + 1)
        base += steps

    for copies in pending:
        sent(copies)
    for p in range(len(PLAN)):
        wait_all(p, stat_send.at[p])


def write_out(basis_ref, tri_ref, basis_out, tri_out, sems):
    copies = (pltpu.make_async_copy(basis_ref, basis_out, sems.at[0]),
              pltpu.make_async_copy(tri_ref, tri_out, sems.at[1]))
    for copy in copies:
        copy.start()
    for copy in copies:
        copy.wait()


def shards(sizes, start_vector, potential):
    Z, Y, X = start_vector.shape
    n = sizes[0] * sizes[1] * sizes[2]
    f32 = jnp.float32
    vmem = pl.BlockSpec(memory_space=pltpu.VMEM)
    hbm = pl.BlockSpec(memory_space=pl.ANY)
    basis, tri = pl.pallas_call(
        functools.partial(kernel, sizes, 1.0 / (start_vector.size * n)),
        out_shape=(pltpu.VMEM((ITERS + 1, Z, Y, X), f32), pltpu.VMEM((2, ITERS), f32)),
        in_specs=[vmem, vmem],
        out_specs=(vmem, vmem),
        scratch_shapes=[
            pltpu.VMEM((ITERS, Z, Y, X), f32),
            pltpu.VMEM((ITERS, 2, Z, X), f32),
            pltpu.VMEM((ITERS, 2, Y, X), f32),
            pltpu.VMEM((ITERS, 2, Z, X), f32),
            pltpu.VMEM((ITERS, Z, Y, X), f32),
            pltpu.VMEM((ITERS, 2, Y, X), f32),
            pltpu.VMEM((ITERS, 2, Z, X), f32),
            pltpu.VMEM((ITERS, Z, Y, X), f32),
            pltpu.VMEM((ITERS, n, 1, X), f32),
            pltpu.SemaphoreType.DMA((ITERS, 5)),
            pltpu.SemaphoreType.DMA((ITERS, 5)),
            pltpu.SemaphoreType.DMA((ITERS,)),
            pltpu.SemaphoreType.DMA((ITERS,)),
        ],
        compiler_params=pltpu.CompilerParams(collective_id=0, has_side_effects=True),
    )(start_vector, potential)
    return tuple(pl.pallas_call(
        write_out,
        out_shape=(jax.ShapeDtypeStruct(basis.shape, f32), jax.ShapeDtypeStruct(tri.shape, f32)),
        in_specs=[vmem, vmem],
        out_specs=(hbm, hbm),
        scratch_shapes=[pltpu.SemaphoreType.DMA((2,))],
    )(pltpu.with_memory_space_constraint(basis, pltpu.VMEM), pltpu.with_memory_space_constraint(tri, pltpu.VMEM)))


def solution(mesh):
    sizes = tuple(mesh.shape[name] for name in AXES)
    in_specs = (P("pz", "py", "slab"), P("pz", "py", "slab"))
    out_specs = (P(None, "pz", "py", "slab"), P())
    return jax.shard_map(functools.partial(shards, sizes), mesh=mesh, in_specs=in_specs,
                         out_specs=out_specs, check_vma=False)
```

```python
import functools

import jax
import jax.numpy as jnp
from jax import lax
from jax.experimental import pallas as pl
from jax.experimental.pallas import tpu as pltpu
from jax.sharding import PartitionSpec as P

ITERS = 5
EPSILON = 1e-06
DIAGONAL = 6.0
FIRST_SHIFTS = (3.5, 10.0)
MESH = pl.DeviceIdType.MESH
AXES = ("slab", "py", "pz")
UNROLLED = 64
PLAN = (2, 3)


def times(coeff, columns):
    total = {}
    for k, c in coeff.items():
        for q, value in columns[k].items():
            term = c * value
            total[q] = total[q] + term if q in total else term
    return total


def dot(left, right):
    total = None
    for q, value in left.items():
        if q in right:
            term = value * right[q]
            total = term if total is None else total + term
    return 0.0 if total is None else total


def advance(j, steps, inner, shifts, taus, removed, betas):
    vectors = [{k: 1.0} for k in range(j + 1)]
    image_of = [{**removed[k], k + 1: betas[k]} for k in range(j)]
    for i in range(steps):
        column = {j + i + 1: 1.0, j + i: shifts[i]}
        if taus[i] is not None:
            column[j + i - 1] = taus[i]
        image_of.append(column)
    gram, lowered = {}, []
    for n in range(j, j + steps):
        for k in range(len(lowered), n + 1):
            lowered.append({
                q: dot(vectors[k], {b: inner[q, b] for b in vectors[k]})
                for q in range(n + 1)})
            for l in range(k + 1):
                gram[k, l] = gram[l, k] = dot(vectors[l], lowered[k])
        known = {n: shifts[n - j]}
        if n > j:
            known[n - 1] = betas[n - 1]
            rest = times(vectors[n], image_of)
            for k, y in known.items():
                for q, value in vectors[k].items():
                    rest[q] = rest[q] - y * value if q in rest else -y * value
        else:
            if taus[0] is not None:
                known[n - 1] = taus[0]
            rest = {n + 1: 1.0}
        rest_lowered = {
            q: dot(rest, {b: inner[q, b] for b in rest}) for q in range(n + 2)}
        along = {k: dot(vectors[k], rest_lowered) for k in range(n + 1)}
        first = {
            k: along[k] + dot(known, {l: gram[k, l] for l in known}) for k in range(n + 1)}
        excess = {k: first[k] - known[k] if k in known else first[k] for k in range(n + 1)}
        coeffs = {
            k: along[k] - dot(excess, {
                l: gram[k, l] - 1.0 if k == l else gram[k, l] for l in range(n + 1)})
            for k in range(n + 1)}
        square = dot(rest, rest_lowered)
        for k in range(n + 1):
            back = dot(coeffs, {l: gram[k, l] for l in range(n + 1)})
            square = square + coeffs[k] * (back - 2.0 * along[k])
        beta = jnp.sqrt(jnp.maximum(square, 0.0) + EPSILON)
        inverse = 1.0 / beta
        image = dict(rest)
        for k in range(n + 1):
            for q, value in vectors[k].items():
                term = coeffs[k] * value
                image[q] = image[q] - term if q in image else -term
        vectors.append({q: value * inverse for q, value in image.items()})
        removed.append({k: coeffs[k] + known[k] if k in known else coeffs[k] for k in coeffs})
        betas.append(beta)
    return vectors[j + 1:]


def basis_of(j, steps, removed, betas, start):
    if j == 0:
        return [start + shift for shift in FIRST_SHIFTS[:steps]], [None] * steps
    shift, beta = removed[j - 1][j - 1], betas[j - 1]
    return [shift] * steps, [beta] + [beta * beta] * (steps - 1)


def kernel(sizes, per_cell, x_hbm, pot_hbm, out_ref, tri_ref, x_ref, pot_ref, work, ysend, zface, yface, xface,
           rz, ry, rx, slots, send_sem, recv_sem, stat_send, stat_recv, load_sem):
    Z, Y, X = x_hbm.shape
    S, A, B = sizes
    n = S * A * B
    slab, py, pz = (lax.axis_index(name) for name in AXES)
    me = (slab * A + py) * B + pz
    partner = lax.rem(slab + 1, S)

    def to_others(act):
        if n <= UNROLLED:
            slabs = [lax.rem(slab + i, S) for i in range(S)]
            pys = [lax.rem(py + i, A) for i in range(A)]
            pzs = [lax.rem(pz + i, B) for i in range(B)]
            far = sorted(
                ((i, j, k) for i in range(S) for j in range(A) for k in range(B)),
                key=lambda t: -(min(t[1], A - t[1]) + min(t[2], B - t[2])),
            )
            for i, j, k in far:
                if i or j or k:
                    act((slabs[i], pys[j], pzs[k]))
        else:
            def step(d, carry):
                t = lax.rem(me + d, n)
                act((t // (A * B), lax.rem(t // B, A), lax.rem(t, B)))
                return carry
            lax.fori_loop(1, n, step, 0)

    def halo_copies(p, zlo, zhi, block):
        def copy(src, dst, side, target):
            return pltpu.make_async_remote_copy(
                src_ref=src, dst_ref=dst, send_sem=send_sem.at[p, side],
                recv_sem=recv_sem.at[p, side], device_id=target, device_id_type=MESH)
        return (
            (pz < B - 1, pz > 0, copy(zhi, rz.at[p, 0], 0, (slab, py, pz + 1))),
            (pz > 0, pz < B - 1, copy(zlo, rz.at[p, 1], 1, (slab, py, pz - 1))),
            (py < A - 1, py > 0, copy(ysend.at[p, 1], ry.at[p, 0], 2, (slab, py + 1, pz))),
            (py > 0, py < A - 1, copy(ysend.at[p, 0], ry.at[p, 1], 3, (slab, py - 1, pz))),
            (None, None, copy(block, rx.at[p], 4, (partner, py, pz))),
        )

    def when(cond, act):
        if cond is None:
            act()
        else:
            pl.when(cond)(act)

    def exchange(p, zlo, zhi, block):
        copies = halo_copies(p, zlo, zhi, block)
        for sends, _, copy in copies:
            when(sends, copy.start)
        return copies

    def arrived(copies):
        for _, receives, copy in copies:
            when(receives, copy.wait_recv)

    def sent(copies):
        for sends, _, copy in copies:
            when(sends, copy.wait_send)

    def stat_copy(p, target):
        return pltpu.make_async_remote_copy(
            src_ref=slots.at[p, me], dst_ref=slots.at[p, me], send_sem=stat_send.at[p],
            recv_sem=stat_recv.at[p], device_id=target, device_id_type=MESH)

    def wait_all(p, sem):
        span = slots.at[p, pl.ds(0, n - 1)]
        pltpu.make_async_copy(span, span, sem).wait()

    lane = lax.broadcasted_iota(jnp.int32, (Y, X), 1)
    row = lax.broadcasted_iota(jnp.int32, (Y, X), 0)
    has_low = (slab > 0).astype(jnp.float32)
    has_high = (slab < S - 1).astype(jnp.float32)

    def stencil(z, own, zf, yf, xf):
        here = own(z)
        below = own(z - 1) if z > 0 else zf(0)
        above = own(z + 1) if z < Z - 1 else zf(1)
        ylow = jnp.where(row == 0, yf(0, z), pltpu.roll(here, 1, 0))
        yhigh = jnp.where(row == Y - 1, yf(1, z), pltpu.roll(here, Y - 1, 0))
        side = xf(z)
        xlow = pltpu.roll(jnp.where(lane == X - 1, side * has_low, here), 1, 1)
        xhigh = pltpu.roll(jnp.where(lane == 0, side * has_high, here), X - 1, 1)
        return (above + below) + (yhigh + ylow) + (xhigh + xlow)

    def fold(value):
        return jnp.sum(value.reshape(Y // 8, 8, X), axis=0)

    def share(p, sums):
        rows = [jnp.sum(v, axis=0, keepdims=True) for v in sums]
        height = -(-len(rows) // 8) * 8
        rows = rows + [jnp.zeros((1, X), jnp.float32)] * (height - len(rows))
        totals = jnp.sum(jnp.concatenate(rows, axis=0), axis=1, keepdims=True)
        at = lax.broadcasted_iota(jnp.int32, (height, X), 0)
        lanes = lax.broadcasted_iota(jnp.int32, (height, X), 1)
        slots[p, me] = jnp.sum(jnp.where(at == lanes, totals, 0.0), axis=0, keepdims=True)
        to_others(lambda target: stat_copy(p, target).start())

    def gathered(p, count):
        wait_all(p, stat_recv.at[p])
        total = jnp.sum(slots[p], axis=0) * per_cell
        return [jnp.broadcast_to(total[:, s:s + 1], (1, X)) for s in range(count)]

    barrier = pltpu.get_barrier_semaphore()
    to_others(lambda t: pl.semaphore_signal(barrier, inc=1, device_id=t, device_id_type=MESH))
    loads = (pltpu.make_async_copy(x_hbm, x_ref, load_sem.at[0]),
             pltpu.make_async_copy(pot_hbm, pot_ref, load_sem.at[1]))
    for load in loads:
        load.start()
    for p in range(ITERS):
        for side, missing in ((0, pz == 0), (1, pz == B - 1)):
            @pl.when(missing)
            def _(p=p, side=side):
                rz[p, side] = jnp.zeros((Y, X), jnp.float32)
        for side, missing in ((0, py == 0), (1, py == A - 1)):
            @pl.when(missing)
            def _(p=p, side=side):
                ry[p, side] = jnp.zeros((Z, X), jnp.float32)
    for load in loads:
        load.wait()
    for z in range(Z):
        ysend[0, 0, z:z + 1] = x_ref[z, 0:1, :]
        ysend[0, 1, z:z + 1] = x_ref[z, Y - 1:Y, :]
    pl.semaphore_wait(barrier, n - 1)

    pending = [exchange(0, x_ref.at[0], x_ref.at[Z - 1], x_ref)]

    def vector(k):
        if k == 0 and base == 0:
            return (lambda z: x_ref[z]), *faces(0)
        return ((lambda z: out_ref[k, z]), (lambda f: zface[k, f]),
                (lambda f, z: yface[k, f, z:z + 1, :]), (lambda z: xface[k, z]),
                (lambda f: yface[k, f]))

    def faces(e):
        return ((lambda f: rz[e, f]), (lambda f, z: ry[e, f, z:z + 1, :]), (lambda z: rx[e, z]),
                (lambda f: ry[e, f]))

    def powered(e):
        return (lambda z: work[e - 1, z]), *faces(e)

    removed, betas, inner, fresh = [], [], {}, range(1)
    start = jnp.zeros((1, X), jnp.float32)
    base, applied = 0, 0
    for phase, steps in enumerate(PLAN):
        last = base + steps == ITERS
        shifts, taus = basis_of(base, steps, removed, betas, start)
        held = [vector(k) for k in range(base + 1)]
        pairs, sums = [], []

        def measure(n, held=held, pairs=pairs, sums=sums):
            totals = [jnp.zeros((8, X), jnp.float32)] * (n + 1)
            for z in range(Z):
                newest = held[n][0](z)
                for k in range(n + 1):
                    totals[k] = totals[k] + fold(held[k][0](z) * newest)
            pairs.extend((k, n) for k in range(n + 1))
            sums.extend(totals)

        if phase == 0:
            for v in fresh:
                measure(v)
            arrived(pending[0])
        for i in range(steps):
            own, zf, yf, xf, _ = held[base + i]
            applied += 1
            ends = applied == ITERS
            for z in range(Z):
                image = (((DIAGONAL - shifts[i]) + pot_ref[z]) * own(z)
                         - stencil(z, own, zf, yf, xf))
                if taus[i] is not None:
                    image = image - taus[i] * held[base + i - 1][0](z)
                work[applied - 1, z] = image
                if not ends:
                    ysend[applied, 0, z:z + 1] = image[0:1]
                    ysend[applied, 1, z:z + 1] = image[Y - 1:Y]
            held.append(powered(applied))
            if not ends:
                pending.append(exchange(applied, work.at[applied - 1, 0],
                                        work.at[applied - 1, Z - 1], work.at[applied - 1]))
            if i == 0 and phase > 0:
                for v in fresh:
                    measure(v)
            measure(base + i + 1)
            if i < steps - 1:
                arrived(pending[applied])
        share(phase, sums)
        stats = gathered(phase, len(sums))
        if phase == 0:
            scale = 1.0 / jnp.sqrt(stats[0] + EPSILON)
            stats = [s * scale * scale for s in stats]
        for (k, l), value in zip(pairs, stats):
            inner[k, l] = inner[l, k] = value
        found = advance(base, steps, inner, shifts, taus, removed, betas)
        for v in range(base, base + steps):
            tri_ref[0:1, v:v + 1] = removed[v][v][:, 0:1]
            tri_ref[1:2, v:v + 1] = betas[v][:, 0:1]
        if phase == 0:
            found = [{q: t * scale for q, t in coords.items()} for coords in found]
        if not last:
            arrived(pending[applied])

        def fill(get, put, only_last):
            columns = [get(held[q]) for q in range(base + steps + 1)]
            if phase == 0 and not (only_last and len(PLAN) == 2):
                put(0, columns[0] * scale)
            for i, coords in enumerate(found):
                if only_last and phase == len(PLAN) - 2 and i < steps - 1:
                    continue
                total = None
                for q in sorted(coords, reverse=True):
                    term = coords[q] * columns[q]
                    total = term if total is None else total + term
                put(base + 1 + i, total)

        def putter(ref, *index):
            def put(k, value):
                ref[(k,) + index] = value
            return put

        for z in range(Z):
            fill(lambda h: h[0](z), putter(out_ref, z), False)
            if not last:
                fill(lambda h: h[3](z), putter(xface, z), True)
        if not last:
            for f in range(2):
                fill(lambda h: h[1](f), putter(zface, f), True)
                fill(lambda h: h[4](f), putter(yface, f), True)
        inner = {pair: value for pair, value in inner.items() if max(pair) <= base}
        fresh = range(base + 1, base + steps + 1)
        base += steps

    for copies in pending:
        sent(copies)
    for p in range(len(PLAN)):
        wait_all(p, stat_send.at[p])


def write_out(basis_ref, tri_ref, basis_out, tri_out, sems):
    copies = (pltpu.make_async_copy(basis_ref, basis_out, sems.at[0]),
              pltpu.make_async_copy(tri_ref, tri_out, sems.at[1]))
    for copy in copies:
        copy.start()
    for copy in copies:
        copy.wait()


def shards(sizes, start_vector, potential):
    Z, Y, X = start_vector.shape
    n = sizes[0] * sizes[1] * sizes[2]
    f32 = jnp.float32
    vmem = pl.BlockSpec(memory_space=pltpu.VMEM)
    hbm = pl.BlockSpec(memory_space=pl.ANY)
    basis, tri = pl.pallas_call(
        functools.partial(kernel, sizes, 1.0 / (start_vector.size * n)),
        out_shape=(pltpu.VMEM((ITERS + 1, Z, Y, X), f32), pltpu.VMEM((2, ITERS), f32)),
        in_specs=[hbm, hbm],
        out_specs=(vmem, vmem),
        scratch_shapes=[
            pltpu.VMEM((Z, Y, X), f32),
            pltpu.VMEM((Z, Y, X), f32),
            pltpu.VMEM((ITERS, Z, Y, X), f32),
            pltpu.VMEM((ITERS, 2, Z, X), f32),
            pltpu.VMEM((ITERS, 2, Y, X), f32),
            pltpu.VMEM((ITERS, 2, Z, X), f32),
            pltpu.VMEM((ITERS, Z, Y, X), f32),
            pltpu.VMEM((ITERS, 2, Y, X), f32),
            pltpu.VMEM((ITERS, 2, Z, X), f32),
            pltpu.VMEM((ITERS, Z, Y, X), f32),
            pltpu.VMEM((ITERS, n, 1, X), f32),
            pltpu.SemaphoreType.DMA((ITERS, 5)),
            pltpu.SemaphoreType.DMA((ITERS, 5)),
            pltpu.SemaphoreType.DMA((ITERS,)),
            pltpu.SemaphoreType.DMA((ITERS,)),
            pltpu.SemaphoreType.DMA((2,)),
        ],
        compiler_params=pltpu.CompilerParams(collective_id=0, has_side_effects=True),
    )(start_vector, potential)
    return tuple(pl.pallas_call(
        write_out,
        out_shape=(jax.ShapeDtypeStruct(basis.shape, f32), jax.ShapeDtypeStruct(tri.shape, f32)),
        in_specs=[vmem, vmem],
        out_specs=(hbm, hbm),
        scratch_shapes=[pltpu.SemaphoreType.DMA((2,))],
    )(pltpu.with_memory_space_constraint(basis, pltpu.VMEM), pltpu.with_memory_space_constraint(tri, pltpu.VMEM)))


def solution(mesh):
    sizes = tuple(mesh.shape[name] for name in AXES)
    in_specs = (P("pz", "py", "slab"), P("pz", "py", "slab"))
    out_specs = (P(None, "pz", "py", "slab"), P())
    return jax.shard_map(functools.partial(shards, sizes), mesh=mesh, in_specs=in_specs,
                         out_specs=out_specs, check_vma=False)
```
